32 devices in a mesh: panel: 4 (over z), rows: 8 (over y, x, core).
Axes of the slice: x: 2, y: 2, z: 4, core: 2. Of those that a mesh axis runs over, the one named last changes fastest.
Arguments:
- rhs_diag: bfloat16 [4, 4096, 128], P(None, 'rows'), may hold values from -6 to 6
- rhs_tall: bfloat16 [4, 4096, 128], P('panel', 'rows'), may hold values from -6 to 6
- diag_inverse: bfloat16 [4, 1024, 1024], P('panel'), may hold values from -0.1875 to 0.1875
- coupling: bfloat16 [4, 4096, 1024], P('panel', 'rows'), may hold values from -0.09375 to 0.09375
- tall_blocks: bfloat16 [4, 32, 128, 1024], P('panel', 'rows'), may hold values from -0.125 to 0.125
- sparsity: int32 [32, 4], P('rows', 'panel'), may hold values 0 or 1
Outputs:
- solution: float32 [4, 4, 1024, 128], P('panel', None, 'rows')
- tall_residual: float32 [4, 4096, 128], P('panel', 'rows')
The draws below stay inside these ranges and needn't reach their ends.
All inputs are finite; a program needn't handle non-finite values. No bound on the sum of `sparsity` on one device may be relied on, other than what follows from the above.
Results may differ from the reference program's by a relative error of at most 0.0085.
Values may be sent and summed in bfloat16 or wider, within the bound.
A program may use at most 64 MiB of HBM per device.

```python
import jax
import jax.numpy as jnp

W = 1024
BLK = 128
RHS = 128
PANELS = 4
BATCHES = 4
ORDER = 4096
NBLK = 32
TALL = 4096


def with_ends(entries, own_key, smallest, top_value):
    longest = entries.shape.index(max(entries.shape))
    spots = []
    for shift in (0, 1):
        where = [jax.random.randint(jax.random.fold_in(own_key, axis), (), 0, length) for axis, length in enumerate(entries.shape)]
        where[longest] = (where[longest] + shift) % entries.shape[longest]
        spots.append(tuple(where))
    return entries.at[spots[0]].set(smallest).at[spots[1]].set(top_value)


def block_scale(rng, shape, split, low, high):
    level = 1.0
    for position, shards_of in split:
        draws = jax.random.uniform(jax.random.fold_in(jax.random.fold_in(rng, 6), position), (shards_of,), jnp.float32, low / len(split), high / len(split))
        level = level * jnp.repeat(jnp.exp(draws), shape[position] // shards_of).reshape((-1,) + (1,) * (len(shape) - 1 - position))
    return level


def scatter_about(rng, dims, width, bound, pieces=(), kind=jnp.bfloat16):
    loudness = block_scale(rng, dims, pieces, -0.22, 0.18) if pieces else 1.0
    values = jax.random.normal(rng, dims, jnp.float32) * width * loudness
    return jnp.minimum(jnp.maximum(values, -bound), bound).astype(kind)


def setup_inputs(seed: int = 0) -> dict:
    key_of = jax.random.split(jax.random.key(seed), 7)
    rhs_diag = scatter_about(key_of[0], (BATCHES, ORDER, RHS), 1.0, 6.0, ((1, 8),))
    rhs_tall = scatter_about(key_of[1], (BATCHES, TALL, RHS), 1.0, 6.0, ((0, 4), (1, 8)))
    diag_inverse = scatter_about(key_of[2], (PANELS, W, W), W ** -0.5, 0.1875, ((0, 4),))
    coupling = scatter_about(key_of[3], (PANELS, ORDER, W), (4 * W) ** -0.5, 0.09375, ((0, 4), (1, 8)))
    tall_blocks = scatter_about(key_of[4], (PANELS, NBLK, BLK, W), (2 * W) ** -0.5, 0.125, ((0, 4), (1, 8)))
    sparsity = with_ends((jax.random.randint(key_of[5], (NBLK, PANELS), 0, 2) < 1).astype(jnp.int32), jax.random.fold_in(key_of[5], 1), 0, 1)
    return {"rhs_diag": rhs_diag, "rhs_tall": rhs_tall, "diag_inverse": diag_inverse, "coupling": coupling, "tall_blocks": tall_blocks, "sparsity": sparsity}


def reference(rhs_diag, rhs_tall, diag_inverse, coupling, tall_blocks, sparsity):
    row_panel = jnp.arange(ORDER, dtype=jnp.int32) // W
    block_mask = jnp.repeat(sparsity.astype(jnp.float32), BLK, axis=0)
    per_batch = []
    for batch_index in range(BATCHES):
        running = jnp.zeros((ORDER, RHS), jnp.float32)
        solved_list = []
        for column_panel in range(PANELS):
            lower = column_panel * W
            rhs_now = rhs_diag[batch_index, lower:lower + W].astype(jnp.float32)
            reduced = (rhs_now - running[lower:lower + W]).astype(jnp.bfloat16)
            solved = jnp.dot(diag_inverse[column_panel], reduced, preferred_element_type=jnp.float32)
            solved_list.append(solved)
            update = jnp.dot(coupling[column_panel], solved.astype(jnp.bfloat16), preferred_element_type=jnp.float32)
            running = running + jnp.where((row_panel > column_panel)[:, None], update, jnp.float32(0.0))
        per_batch.append(jnp.stack(solved_list))
    solution = jnp.stack(per_batch, axis=1)
    tall_sum = jnp.zeros((TALL, BATCHES * RHS), jnp.float32)
    for column_panel in range(PANELS):
        operand = jnp.transpose(solution[column_panel].astype(jnp.bfloat16), (1, 0, 2)).reshape(W, BATCHES * RHS)
        product = jnp.dot(tall_blocks[column_panel].reshape(TALL, W), operand, preferred_element_type=jnp.float32)
        tall_sum = tall_sum + product * block_mask[:, column_panel:column_panel + 1]
    tall_sum = jnp.transpose(tall_sum.reshape(TALL, BATCHES, RHS), (1, 0, 2))
    return solution, rhs_tall.astype(jnp.float32) - tall_sum
```

```python
import functools

import jax
import jax.numpy as jnp
from jax import lax
from jax.experimental import pallas as pl
from jax.experimental.pallas import tpu as pltpu
from jax.sharding import PartitionSpec as P

MESH = pl.DeviceIdType.MESH
CORES = 2


def chain_kernel(
    panels, rhs_ref, tall_rhs_ref, inverse_ref, coupling_ref, tall_ref, mask_ref,
    sol_ref, res_ref,
    inv, cpl, tal, msk, rbuf, tbuf, obuf, xs, xf, ysend, ybuf,
    load_sem, sib_send, sib_recv, first_send, r_sem, t_sem, relay_send, up_send,
    side_send, sol_send, sol_recv, y_send, y_recv,
):
    p = lax.axis_index("panel")
    r = lax.axis_index("rows")
    c = lax.rem(r, CORES)
    j = lax.div(r, CORES)
    sib = r + 1 - 2 * c
    batches, half, _ = rhs_ref.shape
    chips = panels
    steps = batches // CORES
    own_rows = sol_ref.shape[1]
    blocks = mask_ref.shape[0]
    last = panels - 1
    chain = j > p
    feeds_next = j == p + 1
    relays = jnp.logical_and(j == p, p > 0)
    first = jnp.logical_and(p == 0, j == 0)
    next_p = jnp.minimum(p + 1, last)

    def send(src, dst, ssem, rsem, panel, row):
        return pltpu.make_async_remote_copy(
            src_ref=src, dst_ref=dst, send_sem=ssem, recv_sem=rsem,
            device_id=(panel, row), device_id_type=MESH,
        )

    load_inv = pltpu.make_async_copy(inverse_ref, inv, load_sem.at[0])
    load_cpl = pltpu.make_async_copy(coupling_ref, cpl.at[c], load_sem.at[1])
    load_tal = pltpu.make_async_copy(tall_ref, tal.at[c], load_sem.at[2])
    load_msk = pltpu.make_async_copy(mask_ref, msk.at[c], load_sem.at[3])
    for load in (load_inv, load_cpl, load_tal, load_msk):
        load.start()

    def own_rhs(s, into, sem):
        return pltpu.make_async_copy(rhs_ref.at[CORES * s + c], into.at[s, c], sem.at[s, c])

    @pl.when(first)
    def _():
        for s in range(steps):
            own_rhs(s, rbuf, r_sem).start()

    @pl.when(jnp.logical_and(p == 0, j > 0))
    def _():
        for s in range(steps):
            own_rhs(s, tbuf, t_sem).start()

    barrier = pltpu.get_barrier_semaphore()
    for q in range(panels):
        for k in range(CORES):
            @pl.when(jnp.logical_or(q != p, k != c))
            def _():
                pl.semaphore_signal(barrier, inc=1, device_id=(q, CORES * j + k), device_id_type=MESH)
    for i in range(chips):
        for k in range(CORES):
            @pl.when(i != j)
            def _():
                pl.semaphore_signal(barrier, inc=1, device_id=(p, CORES * i + k), device_id_type=MESH)
    side_chip = lax.rem(p + 2, chips)
    gets_side = jnp.logical_and(p > 0, j == lax.rem(p + 1, chips))

    @pl.when(feeds_next)
    def _():
        pl.semaphore_signal(barrier, inc=1, device_id=(next_p, CORES * side_chip + c), device_id_type=MESH)

    @pl.when(gets_side)
    def _():
        pl.semaphore_signal(barrier, inc=1, device_id=(jnp.maximum(p - 1, 0), CORES * p + c), device_id_type=MESH)

    pl.semaphore_wait(
        barrier,
        CORES * panels - 1 + CORES * (chips - 1) + feeds_next.astype(jnp.int32) + gets_side.astype(jnp.int32),
    )

    def first_copies():
        order = [(s, 1) for s in range(steps)] + [(s, i) for i in range(2, chips) for s in range(steps)]
        return [
            send(rhs_ref.at[CORES * s + k], rbuf.at[s, c], first_send.at[s, i, k], r_sem.at[s, c], 0, CORES * i + k)
            for s, i in order for k in range(CORES)
        ]

    def rhs_swap(s, into, sem):
        return send(rhs_ref.at[CORES * s + 1 - c], into.at[s, c], sib_send.at[3 + s], sem.at[s, c], p, sib)

    @pl.when(first)
    def _():
        for copy in first_copies():
            copy.start()
        for s in range(steps):
            rhs_swap(s, rbuf, r_sem).start()

    @pl.when(jnp.logical_and(p == 0, j > 0))
    def _():
        for s in range(steps):
            rhs_swap(s, tbuf, t_sem).start()

    swap_cpl = send(coupling_ref, cpl.at[c], sib_send.at[0], sib_recv.at[0], p, sib)
    swap_tal = send(tall_ref, tal.at[c], sib_send.at[1], sib_recv.at[1], p, sib)
    swap_msk = send(mask_ref, msk.at[c], sib_send.at[2], sib_recv.at[2], p, sib)
    for swap in (swap_cpl, swap_msk, swap_tal):
        swap.start()

    def arrived(ref, sem):
        pltpu.make_async_copy(ref, ref, sem).wait()

    def relay(s, h, n):
        chip = lax.rem(p + 2 + n, chips)
        return send(rbuf.at[s, h], rbuf.at[s, h], relay_send.at[s, h, n], r_sem.at[s, h], p, CORES * chip + c)

    def side(s, h):
        return send(obuf.at[s, h], rbuf.at[s, h], side_send.at[s, h], r_sem.at[s, h], next_p, CORES * side_chip + c)

    def up(s, h, into, sem):
        return send(obuf.at[s, h], into.at[s, h], up_send.at[s, h], sem.at[s, h], next_p, r)

    def sol_copy(s):
        return send(
            xf.at[s, pl.ds(pl.multiple_of(sib * own_rows, own_rows), own_rows)],
            sol_ref.at[CORES * s + c], sol_send.at[s], sol_recv.at[s], p, sib,
        )

    def y_copy(s, h):
        return send(ysend.at[s, h], ybuf.at[p], y_send.at[s, h], y_recv.at[p], CORES * s + c, CORES * j + h)

    def y_local(s, h):
        return jnp.logical_and(CORES * s + c == p, c == h)

    def tall_part(s):
        for h in range(CORES):
            prod = jnp.dot(tal[h], xs[s], preferred_element_type=jnp.float32)
            prod = prod.reshape(blocks, half // blocks, prod.shape[1]) * msk[h][:, 0:1, :]
            ysend[s, h] = prod.reshape(half, prod.shape[2]).astype(jnp.bfloat16)

            @pl.when(jnp.logical_not(y_local(s, h)))
            def _():
                y_copy(s, h).start()

            @pl.when(y_local(s, h))
            def _():
                ybuf[p] = ysend[s, h]

    load_inv.wait()
    for s in range(steps):
        for h in range(CORES):
            arrived(rbuf.at[s, h], r_sem.at[s, h])

            @pl.when(relays)
            def _():
                for n in range(chips - 2):
                    relay(s, h, n).start()

        full = rbuf[s].reshape(inv.shape[1], rbuf.shape[3])
        for h in range(CORES):
            x = jnp.dot(inv[h * half:(h + 1) * half], full, preferred_element_type=jnp.float32)
            xf[s, h * half:(h + 1) * half] = x
            xs[s, h * half:(h + 1) * half] = x.astype(jnp.bfloat16)

        if s == 0:
            load_cpl.wait()
            swap_cpl.wait_recv()

        @pl.when(chain)
        def _():
            for h in range(CORES):
                arrived(tbuf.at[s, h], t_sem.at[s, h])
                update = jnp.dot(cpl[h], xs[s], preferred_element_type=jnp.float32)
                obuf[s, h] = (tbuf[s, h].astype(jnp.float32) - update).astype(jnp.bfloat16)

                @pl.when(feeds_next)
                def _():
                    side(s, h).start()
                    up(s, h, rbuf, r_sem).start()

                @pl.when(jnp.logical_not(feeds_next))
                def _():
                    up(s, h, tbuf, t_sem).start()

        if s == 0:
            load_tal.wait()
            load_msk.wait()
            swap_tal.wait_recv()
            swap_msk.wait_recv()

        sol_ref[CORES * s + c] = xf[s, pl.ds(pl.multiple_of(r * own_rows, own_rows), own_rows)]
        sol_copy(s).start()

        @pl.when(jnp.logical_not(chain))
        def _():
            tall_part(s)

    @pl.when(chain)
    def _():
        for s in range(steps):
            tall_part(s)

    total = tall_rhs_ref[...].astype(jnp.float32)
    for q in range(panels):
        @pl.when(jnp.logical_not(jnp.logical_and(q == p, c == lax.rem(p, CORES))))
        def _():
            arrived(ybuf.at[q], y_recv.at[q])
    for q in range(panels):
        total = total - ybuf[q].astype(jnp.float32)
    res_ref[...] = total

    @pl.when(first)
    def _():
        for copy in first_copies():
            copy.wait_send()
        for s in range(steps):
            rhs_swap(s, rbuf, r_sem).wait_send()

    @pl.when(jnp.logical_and(p == 0, j > 0))
    def _():
        for s in range(steps):
            rhs_swap(s, tbuf, t_sem).wait_send()

    for swap in (swap_cpl, swap_msk, swap_tal):
        swap.wait_send()
    for s in range(steps):
        sol_copy(s).wait_send()
        arrived(sol_ref.at[CORES * s + 1 - c], sol_recv.at[s])
        for h in range(CORES):
            @pl.when(relays)
            def _():
                for n in range(chips - 2):
                    relay(s, h, n).wait_send()

            @pl.when(feeds_next)
            def _():
                side(s, h).wait_send()
                up(s, h, rbuf, r_sem).wait_send()

            @pl.when(jnp.logical_and(chain, jnp.logical_not(feeds_next)))
            def _():
                up(s, h, tbuf, t_sem).wait_send()

            @pl.when(jnp.logical_not(y_local(s, h)))
            def _():
                y_copy(s, h).wait_send()


def chained(rhs_diag, rhs_tall, diag_inverse, coupling, tall_blocks, sparsity):
    panels = lax.axis_size("panel")
    batches, half, columns = rhs_diag.shape
    width = diag_inverse.shape[1]
    own_rows = width // lax.axis_size("rows")
    blocks, block_rows = tall_blocks.shape[1:3]
    tall_rows = blocks * block_rows
    steps = batches // CORES
    mask = jnp.broadcast_to(sparsity[:, 0].astype(jnp.float32)[:, None, None], (blocks, 8, columns))
    anywhere = pl.BlockSpec(memory_space=pl.ANY)
    inside = pl.BlockSpec(memory_space=pltpu.VMEM)
    bf16, f32 = jnp.bfloat16, jnp.float32
    dma = pltpu.SemaphoreType.DMA
    sol, res = pl.pallas_call(
        functools.partial(chain_kernel, panels),
        out_shape=(
            jax.ShapeDtypeStruct((batches, own_rows, columns), f32),
            jax.ShapeDtypeStruct((tall_rows, columns), f32),
        ),
        in_specs=[anywhere, inside, anywhere, anywhere, anywhere, anywhere],
        out_specs=(inside, inside),
        scratch_shapes=[
            pltpu.VMEM((width, width), bf16),
            pltpu.VMEM((CORES, half, width), bf16),
            pltpu.VMEM((CORES, tall_rows, width), bf16),
            pltpu.VMEM((CORES, blocks, 8, columns), f32),
            pltpu.VMEM((steps, CORES, half, columns), bf16),
            pltpu.VMEM((steps, CORES, half, columns), bf16),
            pltpu.VMEM((steps, CORES, half, columns), bf16),
            pltpu.VMEM((steps, width, columns), bf16),
            pltpu.VMEM((steps, width, columns), f32),
            pltpu.VMEM((steps, CORES, tall_rows, columns), bf16),
            pltpu.VMEM((panels, tall_rows, columns), bf16),
            dma((4,)),
            dma((3 + steps,)),
            dma((3,)),
            dma((steps, panels, CORES)),
            dma((steps, CORES)),
            dma((steps, CORES)),
            dma((steps, CORES, max(panels - 2, 1))),
            dma((steps, CORES)),
            dma((steps, CORES)),
            dma((steps,)),
            dma((steps,)),
            dma((steps, CORES)),
            dma((panels,)),
        ],
        compiler_params=pltpu.CompilerParams(
            collective_id=0, has_side_effects=True, vmem_limit_bytes=48 * 1024 * 1024
        ),
    )(rhs_diag, rhs_tall[0], diag_inverse[0], coupling[0], tall_blocks[0].reshape(tall_rows, width), mask)
    return sol[None], res[None]


def fits_chain(mesh, rhs_diag, rhs_tall, diag_inverse, coupling, tall_blocks):
    panels, rows = mesh.shape["panel"], mesh.shape["rows"]
    return (
        rows == CORES * panels
        and rhs_diag.shape[1] == panels * diag_inverse.shape[1]
        and rhs_diag.shape[0] == panels
        and panels % CORES == 0
        and tall_blocks.shape[1] * tall_blocks.shape[2] == rhs_diag.shape[1]
    )


def shifted(block, axis, distance):
    devices = range(lax.axis_size(axis))
    route = [(i - distance, i) for i in devices if i - distance in devices]
    return lax.ppermute(block, axis, route)


def per_device(rhs_diag, rhs_tall, diag_inverse, coupling, tall_blocks, sparsity):
    panel_index = lax.axis_index("panel")
    rows_index = lax.axis_index("rows")
    panel_count = lax.axis_size("panel")
    rows_count = lax.axis_size("rows")
    batches, rows_here, columns = rhs_diag.shape
    panel_width = diag_inverse.shape[1]
    slice_rows = panel_width // rows_count
    blocks_here = tall_blocks.shape[1]
    block_rows = tall_blocks.shape[2]
    tall_rows = blocks_here * block_rows
    rows_panel = rows_index * rows_here // panel_width
    offset = jnp.clip(
        rows_index * rows_here - panel_index * panel_width, 0, panel_width - rows_here
    )
    inverse_cols = lax.dynamic_slice_in_dim(diag_inverse[0], offset, rows_here, 1)
    owner = rows_panel == panel_index
    is_later = rows_panel > panel_index
    coupling_here = coupling[0]
    tall_matrix = tall_blocks[0].reshape(tall_rows, panel_width)
    block_mask = jnp.repeat(sparsity[:, 0].astype(jnp.float32), block_rows)[:, None]

    def advance(tick_number, state_now):
        incoming, solutions, stored = state_now
        batch_now = tick_number - panel_index
        active = (batch_now >= 0) & (batch_now < batches)
        batch_safe = jnp.clip(batch_now, 0, batches - 1)
        rhs_now = lax.dynamic_index_in_dim(rhs_diag, batch_safe, 0, keepdims=False).astype(
            jnp.float32
        )
        reduced = (rhs_now - incoming).astype(jnp.bfloat16)
        partial_value = jnp.dot(inverse_cols, reduced, preferred_element_type=jnp.float32)
        partial_value = jnp.where(owner, partial_value, jnp.float32(0.0))
        own_rows = lax.psum_scatter(partial_value, "rows", scatter_dimension=0, tiled=True)
        solved = lax.all_gather(own_rows.astype(jnp.bfloat16), "rows", axis=0, tiled=True)
        previous = lax.dynamic_index_in_dim(solutions, batch_safe, 0, keepdims=False)
        solutions = lax.dynamic_update_index_in_dim(
            solutions, jnp.where(active, own_rows, previous), batch_safe, 0
        )
        update = jnp.dot(coupling_here, solved, preferred_element_type=jnp.float32)
        outgoing = incoming + jnp.where(is_later, update, jnp.float32(0.0))
        earlier = lax.dynamic_index_in_dim(stored, batch_safe, 0, keepdims=False)
        stored = lax.dynamic_update_index_in_dim(
            stored, jnp.where(active, solved, earlier), batch_safe, 0
        )
        incoming = shifted(outgoing, "panel", 1)
        return (incoming, solutions, stored)

    stored = jnp.zeros((batches, panel_width, columns), jnp.bfloat16)
    initial = (
        jnp.zeros((rows_here, columns), jnp.float32),
        jnp.zeros((batches, slice_rows, columns), jnp.float32),
        stored,
    )
    tick_count = batches + panel_count - 1
    incoming, solutions, stored = lax.fori_loop(0, tick_count, advance, initial)
    tall_terms = (
        jnp.einsum("rw,bws->brs", tall_matrix, stored, preferred_element_type=jnp.float32)
        * block_mask
    )
    summed = lax.psum_scatter(tall_terms, "panel", scatter_dimension=0, tiled=True)
    tall_residual = rhs_tall.astype(jnp.float32) - summed
    return (solutions[None], tall_residual)


def solution(mesh):
    placed = (
        P(None, "rows", None),
        P("panel", "rows", None),
        P("panel", None, None),
        P("panel", "rows", None),
        P("panel", "rows", None, None),
        P("rows", "panel"),
    )

    def run(*arrays):
        body = chained if fits_chain(mesh, *arrays[:5]) else per_device
        return jax.shard_map(
            body,
            mesh=mesh,
            in_specs=placed,
            out_specs=(P("panel", None, "rows", None), P("panel", "rows", None)),
            check_vma=False,
        )(*arrays)

    return run
```

```python
import functools

import jax
import jax.numpy as jnp
from jax import lax
from jax.experimental import pallas as pl
from jax.experimental.pallas import tpu as pltpu
from jax.sharding import PartitionSpec as P

MESH = pl.DeviceIdType.MESH
CORES = 2


def chain_kernel(
    panels, rhs_ref, tall_rhs_ref, inverse_ref, coupling_ref, tall_ref, mask_ref,
    sol_ref, res_ref,
    inv, cpl, tal, msk, rhs, rbuf, tbuf, obuf, xs, xf, ysend, ybuf,
    load_sem, sib_send, sib_recv, swap_send, r_sem, t_sem, relay_send, up_send,
    sol_send, sol_recv, y_send, y_recv,
):
    p = lax.axis_index("panel")
    r = lax.axis_index("rows")
    c = lax.rem(r, CORES)
    j = lax.div(r, CORES)
    sib = r + 1 - 2 * c
    batches, half, _ = rhs_ref.shape
    chips = panels
    steps = batches // CORES
    parts, part_rows = rbuf.shape[1:3]
    own_parts = parts // CORES
    levels = chips.bit_length() - 1
    own_rows = sol_ref.shape[1]
    blocks = mask_ref.shape[0]
    last = panels - 1
    chain = j > p
    feeds_next = j == p + 1
    next_p = jnp.minimum(p + 1, last)
    next_root = jnp.minimum(p + 2, last)
    root = jnp.where(p == 0, 0, jnp.minimum(p + 1, last))
    place = jnp.bitwise_xor(j, root)
    first = jnp.logical_and(p == 0, j == 0)
    later = jnp.logical_and(p == 0, j > 0)

    def send(src, dst, ssem, rsem, panel, row):
        return pltpu.make_async_remote_copy(
            src_ref=src, dst_ref=dst, send_sem=ssem, recv_sem=rsem,
            device_id=(panel, row), device_id_type=MESH,
        )

    load_inv = pltpu.make_async_copy(inverse_ref, inv, load_sem.at[0])
    load_cpl = pltpu.make_async_copy(coupling_ref, cpl.at[c], load_sem.at[1])
    load_tal = pltpu.make_async_copy(tall_ref, tal.at[c], load_sem.at[2])
    load_msk = pltpu.make_async_copy(mask_ref, msk.at[c], load_sem.at[3])
    load_rhs = pltpu.make_async_copy(tall_rhs_ref, rhs, load_sem.at[4])

    def own_rhs(s, i, into, sem):
        part = c * own_parts + i
        return pltpu.make_async_copy(
            rhs_ref.at[CORES * s + c, pl.ds(i * part_rows, part_rows)], into.at[s, part], sem.at[s, part]
        )

    pieces = [(s, i) for s in range(steps) for i in range(own_parts)]

    @pl.when(first)
    def _():
        for s, i in pieces:
            own_rhs(s, i, rbuf, r_sem).start()

    @pl.when(later)
    def _():
        for s, i in pieces:
            own_rhs(s, i, tbuf, t_sem).start()

    for load in (load_inv, load_cpl, load_tal, load_msk, load_rhs):
        load.start()

    barrier = pltpu.get_barrier_semaphore()
    for q in range(panels):
        for k in range(CORES):
            @pl.when(jnp.logical_or(q != p, k != c))
            def _():
                pl.semaphore_signal(barrier, inc=1, device_id=(q, CORES * j + k), device_id_type=MESH)
    for i in range(chips):
        for k in range(CORES):
            @pl.when(i != j)
            def _():
                pl.semaphore_signal(barrier, inc=1, device_id=(p, CORES * i + k), device_id_type=MESH)
    leaves = jnp.logical_and(feeds_next, next_root != j)
    enters = jnp.logical_and(jnp.logical_and(p > 0, j == root), root != p)

    @pl.when(leaves)
    def _():
        pl.semaphore_signal(barrier, inc=1, device_id=(next_p, CORES * next_root + c), device_id_type=MESH)

    @pl.when(enters)
    def _():
        pl.semaphore_signal(barrier, inc=1, device_id=(jnp.maximum(p - 1, 0), CORES * p + c), device_id_type=MESH)

    pl.semaphore_wait(
        barrier,
        CORES * panels - 1 + CORES * (chips - 1) + leaves.astype(jnp.int32) + enters.astype(jnp.int32),
    )

    def rhs_swap(s, i, into, sem):
        part = c * own_parts + i
        return send(
            rhs_ref.at[CORES * s + 1 - c, pl.ds(i * part_rows, part_rows)], into.at[s, part],
            swap_send.at[s, i], sem.at[s, part], p, sib,
        )

    @pl.when(first)
    def _():
        for s, i in pieces:
            rhs_swap(s, i, rbuf, r_sem).start()

    @pl.when(later)
    def _():
        for s, i in pieces:
            rhs_swap(s, i, tbuf, t_sem).start()

    swap_cpl = send(coupling_ref, cpl.at[c], sib_send.at[0], sib_recv.at[0], p, sib)
    swap_tal = send(tall_ref, tal.at[c], sib_send.at[1], sib_recv.at[1], p, sib)
    swap_msk = send(mask_ref, msk.at[c], sib_send.at[2], sib_recv.at[2], p, sib)
    for swap in (swap_cpl, swap_msk, swap_tal):
        swap.start()

    def arrived(ref, sem):
        pltpu.make_async_copy(ref, ref, sem).wait()

    def relay(s, part, level):
        chip = jnp.bitwise_xor(j, 1 << level)
        return send(
            rbuf.at[s, part], rbuf.at[s, part], relay_send.at[s, part, level], r_sem.at[s, part],
            p, CORES * chip + c,
        )

    def relays(level):
        return lax.rem(place, 2 << level) == 0

    def ahead(s, part):
        return send(
            obuf.at[s, part], rbuf.at[s, part], up_send.at[s, part], r_sem.at[s, part],
            next_p, CORES * next_root + c,
        )

    def up(s, part):
        return send(obuf.at[s, part], tbuf.at[s, part], up_send.at[s, part], t_sem.at[s, part], next_p, r)

    def sol_copy(s):
        return send(
            xf.at[s, pl.ds(pl.multiple_of(sib * own_rows, own_rows), own_rows)],
            sol_ref.at[CORES * s + c], sol_send.at[s], sol_recv.at[s], p, sib,
        )

    def y_copy(s, h):
        return send(ysend.at[s, h], ybuf.at[p], y_send.at[s, h], y_recv.at[p], CORES * s + c, CORES * j + h)

    def y_local(s, h):
        return jnp.logical_and(CORES * s + c == p, c == h)

    def tall_part(s):
        for h in range(CORES):
            prod = jnp.dot(tal[h], xs[s], preferred_element_type=jnp.float32)
            prod = prod.reshape(blocks, half // blocks, prod.shape[1]) * msk[h][:, 0:1, :]
            ysend[s, h] = prod.reshape(half, prod.shape[2]).astype(jnp.bfloat16)

            @pl.when(jnp.logical_not(y_local(s, h)))
            def _():
                y_copy(s, h).start()

            @pl.when(y_local(s, h))
            def _():
                ybuf[p] = ysend[s, h]

    turn = jnp.where(p == 0, c * own_parts, 0)
    for s in range(steps):
        for i in range(parts):
            part = lax.rem(i + turn, parts)
            arrived(rbuf.at[s, part], r_sem.at[s, part])
            for level in range(levels):
                @pl.when(relays(level))
                def _():
                    relay(s, part, level).start()

        if s == 0:
            load_inv.wait()
        full = rbuf[s].reshape(inv.shape[1], rbuf.shape[3])
        for h in range(CORES):
            x = jnp.dot(inv[h * half:(h + 1) * half], full, preferred_element_type=jnp.float32)
            xf[s, h * half:(h + 1) * half] = x
            xs[s, h * half:(h + 1) * half] = x.astype(jnp.bfloat16)

        if s == 0:
            load_cpl.wait()
            swap_cpl.wait_recv()

        @pl.when(chain)
        def _():
            for part in range(parts):
                h, i = divmod(part, own_parts)
                arrived(tbuf.at[s, part], t_sem.at[s, part])
                update = jnp.dot(
                    cpl[h, i * part_rows:(i + 1) * part_rows], xs[s], preferred_element_type=jnp.float32
                )
                obuf[s, part] = (tbuf[s, part].astype(jnp.float32) - update).astype(jnp.bfloat16)

                @pl.when(feeds_next)
                def _():
                    ahead(s, part).start()

                @pl.when(jnp.logical_not(feeds_next))
                def _():
                    up(s, part).start()

        if s == 0:
            load_tal.wait()
            load_msk.wait()
            swap_tal.wait_recv()
            swap_msk.wait_recv()

        sol_ref[CORES * s + c] = xf[s, pl.ds(pl.multiple_of(r * own_rows, own_rows), own_rows)]
        sol_copy(s).start()

        @pl.when(jnp.logical_not(chain))
        def _():
            tall_part(s)

    @pl.when(chain)
    def _():
        for s in range(steps):
            tall_part(s)

    load_rhs.wait()
    total = rhs[...].astype(jnp.float32)
    for q in range(panels):
        @pl.when(jnp.logical_not(jnp.logical_and(q == p, c == lax.rem(p, CORES))))
        def _():
            arrived(ybuf.at[q], y_recv.at[q])
    for q in range(panels):
        total = total - ybuf[q].astype(jnp.float32)
    res_ref[...] = total

    @pl.when(p == 0)
    def _():
        for s, i in pieces:
            rhs_swap(s, i, rbuf, r_sem).wait_send()

    for swap in (swap_cpl, swap_msk, swap_tal):
        swap.wait_send()
    for s in range(steps):
        sol_copy(s).wait_send()
        arrived(sol_ref.at[CORES * s + 1 - c], sol_recv.at[s])
        for part in range(parts):
            for level in range(levels):
                @pl.when(relays(level))
                def _():
                    relay(s, part, level).wait_send()

            @pl.when(chain)
            def _():
                ahead(s, part).wait_send()

        for h in range(CORES):
            @pl.when(jnp.logical_not(y_local(s, h)))
            def _():
                y_copy(s, h).wait_send()


def chained(rhs_diag, rhs_tall, diag_inverse, coupling, tall_blocks, sparsity):
    panels = lax.axis_size("panel")
    batches, half, columns = rhs_diag.shape
    width = diag_inverse.shape[1]
    own_rows = width // lax.axis_size("rows")
    blocks, block_rows = tall_blocks.shape[1:3]
    tall_rows = blocks * block_rows
    steps = batches // CORES
    mask = jnp.broadcast_to(sparsity[:, 0].astype(jnp.float32)[:, None, None], (blocks, 8, columns))
    parts = 2 * CORES
    part_rows = width // parts
    anywhere = pl.BlockSpec(memory_space=pltpu.HBM)
    inside = pl.BlockSpec(memory_space=pltpu.VMEM)
    bf16, f32 = jnp.bfloat16, jnp.float32
    dma = pltpu.SemaphoreType.DMA
    sol, res = pl.pallas_call(
        functools.partial(chain_kernel, panels),
        out_shape=(
            jax.ShapeDtypeStruct((batches, own_rows, columns), f32),
            jax.ShapeDtypeStruct((tall_rows, columns), f32),
        ),
        in_specs=[anywhere] * 6,
        out_specs=(inside, inside),
        scratch_shapes=[
            pltpu.VMEM((width, width), bf16),
            pltpu.VMEM((CORES, half, width), bf16),
            pltpu.VMEM((CORES, tall_rows, width), bf16),
            pltpu.VMEM((CORES, blocks, 8, columns), f32),
            pltpu.VMEM((tall_rows, columns), bf16),
            pltpu.VMEM((steps, parts, part_rows, columns), bf16),
            pltpu.VMEM((steps, parts, part_rows, columns), bf16),
            pltpu.VMEM((steps, parts, part_rows, columns), bf16),
            pltpu.VMEM((steps, width, columns), bf16),
            pltpu.VMEM((steps, width, columns), f32),
            pltpu.VMEM((steps, CORES, tall_rows, columns), bf16),
            pltpu.VMEM((panels, tall_rows, columns), bf16),
            dma((5,)),
            dma((3,)),
            dma((3,)),
            dma((steps, parts // CORES)),
            dma((steps, parts)),
            dma((steps, parts)),
            dma((steps, parts, panels.bit_length())),
            dma((steps, parts)),
            dma((steps,)),
            dma((steps,)),
            dma((steps, CORES)),
            dma((panels,)),
        ],
        compiler_params=pltpu.CompilerParams(
            collective_id=0, has_side_effects=True, vmem_limit_bytes=67_043_328
        ),
    )(rhs_diag, rhs_tall[0], diag_inverse[0], coupling[0], tall_blocks[0].reshape(tall_rows, width), mask)
    return sol[None], res[None]


def fits_chain(mesh, rhs_diag, rhs_tall, diag_inverse, coupling, tall_blocks):
    panels, rows = mesh.shape["panel"], mesh.shape["rows"]
    return (
        rows == CORES * panels
        and rhs_diag.shape[1] == panels * diag_inverse.shape[1]
        and rhs_diag.shape[0] == panels
        and panels % CORES == 0
        and panels & (panels - 1) == 0
        and tall_blocks.shape[1] * tall_blocks.shape[2] == rhs_diag.shape[1]
    )


def shifted(block, axis, distance):
    devices = range(lax.axis_size(axis))
    route = [(i - distance, i) for i in devices if i - distance in devices]
    return lax.ppermute(block, axis, route)


def per_device(rhs_diag, rhs_tall, diag_inverse, coupling, tall_blocks, sparsity):
    panel_index = lax.axis_index("panel")
    rows_index = lax.axis_index("rows")
    panel_count = lax.axis_size("panel")
    rows_count = lax.axis_size("rows")
    batches, rows_here, columns = rhs_diag.shape
    panel_width = diag_inverse.shape[1]
    slice_rows = panel_width // rows_count
    blocks_here = tall_blocks.shape[1]
    block_rows = tall_blocks.shape[2]
    tall_rows = blocks_here * block_rows
    rows_panel = rows_index * rows_here // panel_width
    offset = jnp.clip(
        rows_index * rows_here - panel_index * panel_width, 0, panel_width - rows_here
    )
    inverse_cols = lax.dynamic_slice_in_dim(diag_inverse[0], offset, rows_here, 1)
    owner = rows_panel == panel_index
    is_later = rows_panel > panel_index
    coupling_here = coupling[0]
    tall_matrix = tall_blocks[0].reshape(tall_rows, panel_width)
    block_mask = jnp.repeat(sparsity[:, 0].astype(jnp.float32), block_rows)[:, None]

    def advance(tick_number, state_now):
        incoming, solutions, stored = state_now
        batch_now = tick_number - panel_index
        active = (batch_now >= 0) & (batch_now < batches)
        batch_safe = jnp.clip(batch_now, 0, batches - 1)
        rhs_now = lax.dynamic_index_in_dim(rhs_diag, batch_safe, 0, keepdims=False).astype(
            jnp.float32
        )
        reduced = (rhs_now - incoming).astype(jnp.bfloat16)
        partial_value = jnp.dot(inverse_cols, reduced, preferred_element_type=jnp.float32)
        partial_value = jnp.where(owner, partial_value, jnp.float32(0.0))
        own_rows = lax.psum_scatter(partial_value, "rows", scatter_dimension=0, tiled=True)
        solved = lax.all_gather(own_rows.astype(jnp.bfloat16), "rows", axis=0, tiled=True)
        previous = lax.dynamic_index_in_dim(solutions, batch_safe, 0, keepdims=False)
        solutions = lax.dynamic_update_index_in_dim(
            solutions, jnp.where(active, own_rows, previous), batch_safe, 0
        )
        update = jnp.dot(coupling_here, solved, preferred_element_type=jnp.float32)
        outgoing = incoming + jnp.where(is_later, update, jnp.float32(0.0))
        earlier = lax.dynamic_index_in_dim(stored, batch_safe, 0, keepdims=False)
        stored = lax.dynamic_update_index_in_dim(
            stored, jnp.where(active, solved, earlier), batch_safe, 0
        )
        incoming = shifted(outgoing, "panel", 1)
        return (incoming, solutions, stored)

    stored = jnp.zeros((batches, panel_width, columns), jnp.bfloat16)
    initial = (
        jnp.zeros((rows_here, columns), jnp.float32),
        jnp.zeros((batches, slice_rows, columns), jnp.float32),
        stored,
    )
    tick_count = batches + panel_count - 1
    incoming, solutions, stored = lax.fori_loop(0, tick_count, advance, initial)
    tall_terms = (
        jnp.einsum("rw,bws->brs", tall_matrix, stored, preferred_element_type=jnp.float32)
        * block_mask
    )
    summed = lax.psum_scatter(tall_terms, "panel", scatter_dimension=0, tiled=True)
    tall_residual = rhs_tall.astype(jnp.float32) - summed
    return (solutions[None], tall_residual)


def solution(mesh):
    placed = (
        P(None, "rows", None),
        P("panel", "rows", None),
        P("panel", None, None),
        P("panel", "rows", None),
        P("panel", "rows", None, None),
        P("rows", "panel"),
    )

    def run(*arrays):
        body = chained if fits_chain(mesh, *arrays[:5]) else per_device
        return jax.shard_map(
            body,
            mesh=mesh,
            in_specs=placed,
            out_specs=(P("panel", None, "rows", None), P("panel", "rows", None)),
            check_vma=False,
        )(*arrays)

    return run
```

```python
import functools

import jax
import jax.numpy as jnp
from jax import lax
from jax.experimental import pallas as pl
from jax.experimental.pallas import tpu as pltpu
from jax.sharding import PartitionSpec as P

MESH = pl.DeviceIdType.MESH
CORES = 2


def chain_kernel(
    panels, rhs_ref, tall_rhs_ref, inverse_ref, coupling_ref, tall_ref, mask_ref,
    sol_ref, res_ref,
    inv, cpl, tal, msk, rhs, rbuf, tbuf, obuf, xs, xf, ysend, ybuf,
    load_sem, sib_send, sib_recv, swap_send, first_send, r_sem, t_sem, relay_send, up_send,
    sol_send, sol_recv, y_send, y_recv,
):
    p = lax.axis_index("panel")
    r = lax.axis_index("rows")
    c = lax.rem(r, CORES)
    j = lax.div(r, CORES)
    sib = r + 1 - 2 * c
    batches, half, _ = rhs_ref.shape
    chips = panels
    steps = batches // CORES
    parts, part_rows = rbuf.shape[1:3]
    own_parts = parts // CORES
    levels = chips.bit_length() - 1
    own_rows = sol_ref.shape[1]
    blocks = mask_ref.shape[0]
    last = panels - 1
    chain = j > p
    feeds_next = j == p + 1
    next_p = jnp.minimum(p + 1, last)
    next_root = jnp.minimum(p + 2, last)
    root = jnp.where(p == 0, 0, jnp.minimum(p + 1, last))
    place = jnp.bitwise_xor(j, root)
    first = jnp.logical_and(p == 0, j == 0)
    later = jnp.logical_and(p == 0, j > 0)

    def send(src, dst, ssem, rsem, panel, row):
        return pltpu.make_async_remote_copy(
            src_ref=src, dst_ref=dst, send_sem=ssem, recv_sem=rsem,
            device_id=(panel, row), device_id_type=MESH,
        )

    load_inv = pltpu.make_async_copy(inverse_ref, inv, load_sem.at[0])
    load_cpl = pltpu.make_async_copy(coupling_ref, cpl.at[c], load_sem.at[1])
    load_tal = pltpu.make_async_copy(tall_ref, tal.at[c], load_sem.at[2])
    load_msk = pltpu.make_async_copy(mask_ref, msk.at[c], load_sem.at[3])
    load_rhs = pltpu.make_async_copy(tall_rhs_ref, rhs, load_sem.at[4])

    def own_rhs(s, i, into, sem):
        part = c * own_parts + i
        return pltpu.make_async_copy(
            rhs_ref.at[CORES * s + c, pl.ds(i * part_rows, part_rows)], into.at[s, part], sem.at[s, part]
        )

    pieces = [(s, i) for s in range(steps) for i in range(own_parts)]

    @pl.when(first)
    def _():
        for s, i in pieces:
            own_rhs(s, i, rbuf, r_sem).start()

    @pl.when(later)
    def _():
        for s, i in pieces:
            own_rhs(s, i, tbuf, t_sem).start()

    for load in (load_inv, load_cpl, load_tal, load_msk, load_rhs):
        load.start()

    barrier = pltpu.get_barrier_semaphore()
    for q in range(panels):
        for k in range(CORES):
            @pl.when(jnp.logical_or(q != p, k != c))
            def _():
                pl.semaphore_signal(barrier, inc=1, device_id=(q, CORES * j + k), device_id_type=MESH)
    for i in range(chips):
        for k in range(CORES):
            @pl.when(i != j)
            def _():
                pl.semaphore_signal(barrier, inc=1, device_id=(p, CORES * i + k), device_id_type=MESH)
    leaves = jnp.logical_and(feeds_next, next_root != j)
    enters = jnp.logical_and(jnp.logical_and(p > 0, j == root), root != p)

    @pl.when(leaves)
    def _():
        pl.semaphore_signal(barrier, inc=1, device_id=(next_p, CORES * next_root + c), device_id_type=MESH)

    @pl.when(enters)
    def _():
        pl.semaphore_signal(barrier, inc=1, device_id=(jnp.maximum(p - 1, 0), CORES * p + c), device_id_type=MESH)

    pl.semaphore_wait(
        barrier,
        CORES * panels - 1 + CORES * (chips - 1) + leaves.astype(jnp.int32) + enters.astype(jnp.int32),
    )

    def rhs_swap(s, i, into, sem):
        part = c * own_parts + i
        return send(
            rhs_ref.at[CORES * s + 1 - c, pl.ds(i * part_rows, part_rows)], into.at[s, part],
            swap_send.at[s, i], sem.at[s, part], p, sib,
        )

    def outward(k, level, i):
        part = c * own_parts + i
        return send(
            rhs_ref.at[k, pl.ds(i * part_rows, part_rows)], rbuf.at[k // CORES, part],
            first_send.at[k, level, i], r_sem.at[k // CORES, part], p, (CORES << level) + k % CORES,
        )

    outwards = [(k, n, i) for k in range(batches) for n in range(levels) for i in range(own_parts)]

    @pl.when(first)
    def _():
        for k, level, i in outwards:
            outward(k, level, i).start()
        for s, i in pieces:
            rhs_swap(s, i, rbuf, r_sem).start()

    @pl.when(later)
    def _():
        for s, i in pieces:
            rhs_swap(s, i, tbuf, t_sem).start()

    swap_cpl = send(coupling_ref, cpl.at[c], sib_send.at[0], sib_recv.at[0], p, sib)
    swap_tal = send(tall_ref, tal.at[c], sib_send.at[1], sib_recv.at[1], p, sib)
    swap_msk = send(mask_ref, msk.at[c], sib_send.at[2], sib_recv.at[2], p, sib)
    for swap in (swap_cpl, swap_msk, swap_tal):
        swap.start()

    def arrived(ref, sem):
        pltpu.make_async_copy(ref, ref, sem).wait()

    def relay(s, part, level):
        chip = jnp.bitwise_xor(j, 1 << level)
        return send(
            rbuf.at[s, part], rbuf.at[s, part], relay_send.at[s, part, level], r_sem.at[s, part],
            p, CORES * chip + c,
        )

    def relays(level):
        return jnp.logical_and(lax.rem(place, 2 << level) == 0, jnp.logical_not(first))

    def ahead(s, part):
        return send(
            obuf.at[s, part], rbuf.at[s, part], up_send.at[s, part], r_sem.at[s, part],
            next_p, CORES * next_root + c,
        )

    def up(s, part):
        return send(obuf.at[s, part], tbuf.at[s, part], up_send.at[s, part], t_sem.at[s, part], next_p, r)

    def sol_copy(s):
        return send(
            xf.at[s, pl.ds(pl.multiple_of(sib * own_rows, own_rows), own_rows)],
            sol_ref.at[CORES * s + c], sol_send.at[s], sol_recv.at[s], p, sib,
        )

    def y_copy(s, h):
        return send(ysend.at[s, h], ybuf.at[p], y_send.at[s, h], y_recv.at[p], CORES * s + c, CORES * j + h)

    def y_local(s, h):
        return jnp.logical_and(CORES * s + c == p, c == h)

    def tall_part(s):
        for h in range(CORES):
            prod = jnp.dot(tal[h], xs[s], preferred_element_type=jnp.float32)
            prod = prod.reshape(blocks, half // blocks, prod.shape[1]) * msk[h][:, 0:1, :]
            ysend[s, h] = prod.reshape(half, prod.shape[2]).astype(jnp.bfloat16)

            @pl.when(jnp.logical_not(y_local(s, h)))
            def _():
                y_copy(s, h).start()

            @pl.when(y_local(s, h))
            def _():
                ybuf[p] = ysend[s, h]

    load_inv.wait()
    for s in range(steps):
        for part in range(parts):
            arrived(rbuf.at[s, part], r_sem.at[s, part])
            for level in range(levels):
                @pl.when(relays(level))
                def _():
                    relay(s, part, level).start()

            x = jnp.dot(
                inv[:, part * part_rows:(part + 1) * part_rows], rbuf[s, part], preferred_element_type=jnp.float32
            )
            xf[s] = x if part == 0 else xf[s] + x
        xs[s] = xf[s].astype(jnp.bfloat16)

        if s == 0:
            load_cpl.wait()
            swap_cpl.wait_recv()

        @pl.when(chain)
        def _():
            for part in range(parts):
                h, i = divmod(part, own_parts)
                arrived(tbuf.at[s, part], t_sem.at[s, part])
                update = jnp.dot(
                    cpl[h, i * part_rows:(i + 1) * part_rows], xs[s], preferred_element_type=jnp.float32
                )
                obuf[s, part] = (tbuf[s, part].astype(jnp.float32) - update).astype(jnp.bfloat16)

                @pl.when(feeds_next)
                def _():
                    ahead(s, part).start()

                @pl.when(jnp.logical_not(feeds_next))
                def _():
                    up(s, part).start()

        if s == 0:
            load_tal.wait()
            load_msk.wait()
            swap_tal.wait_recv()
            swap_msk.wait_recv()

        sol_ref[CORES * s + c] = xf[s, pl.ds(pl.multiple_of(r * own_rows, own_rows), own_rows)]
        sol_copy(s).start()

        @pl.when(jnp.logical_not(chain))
        def _():
            tall_part(s)

    @pl.when(chain)
    def _():
        for s in range(steps):
            tall_part(s)

    load_rhs.wait()
    total = rhs[...].astype(jnp.float32)
    for q in range(panels):
        @pl.when(jnp.logical_not(jnp.logical_and(q == p, c == lax.rem(p, CORES))))
        def _():
            arrived(ybuf.at[q], y_recv.at[q])
    for q in range(panels):
        total = total - ybuf[q].astype(jnp.float32)
    res_ref[...] = total

    @pl.when(p == 0)
    def _():
        for s, i in pieces:
            rhs_swap(s, i, rbuf, r_sem).wait_send()

    @pl.when(first)
    def _():
        for k, level, i in outwards:
            outward(k, level, i).wait_send()

    for swap in (swap_cpl, swap_msk, swap_tal):
        swap.wait_send()
    for s in range(steps):
        sol_copy(s).wait_send()
        arrived(sol_ref.at[CORES * s + 1 - c], sol_recv.at[s])
        for part in range(parts):
            for level in range(levels):
                @pl.when(relays(level))
                def _():
                    relay(s, part, level).wait_send()

            @pl.when(chain)
            def _():
                ahead(s, part).wait_send()

        for h in range(CORES):
            @pl.when(jnp.logical_not(y_local(s, h)))
            def _():
                y_copy(s, h).wait_send()


def chained(rhs_diag, rhs_tall, diag_inverse, coupling, tall_blocks, sparsity):
    panels = lax.axis_size("panel")
    batches, half, columns = rhs_diag.shape
    width = diag_inverse.shape[1]
    own_rows = width // lax.axis_size("rows")
    blocks, block_rows = tall_blocks.shape[1:3]
    tall_rows = blocks * block_rows
    steps = batches // CORES
    mask = jnp.broadcast_to(sparsity[:, 0].astype(jnp.float32)[:, None, None], (blocks, 8, columns))
    parts = 2 * CORES
    part_rows = width // parts
    anywhere = pl.BlockSpec(memory_space=pltpu.HBM)
    inside = pl.BlockSpec(memory_space=pltpu.VMEM)
    bf16, f32 = jnp.bfloat16, jnp.float32
    dma = pltpu.SemaphoreType.DMA
    sol, res = pl.pallas_call(
        functools.partial(chain_kernel, panels),
        out_shape=(
            jax.ShapeDtypeStruct((batches, own_rows, columns), f32),
            jax.ShapeDtypeStruct((tall_rows, columns), f32),
        ),
        in_specs=[anywhere] * 6,
        out_specs=(inside, inside),
        scratch_shapes=[
            pltpu.VMEM((width, width), bf16),
            pltpu.VMEM((CORES, half, width), bf16),
            pltpu.VMEM((CORES, tall_rows, width), bf16),
            pltpu.VMEM((CORES, blocks, 8, columns), f32),
            pltpu.VMEM((tall_rows, columns), bf16),
            pltpu.VMEM((steps, parts, part_rows, columns), bf16),
            pltpu.VMEM((steps, parts, part_rows, columns), bf16),
            pltpu.VMEM((steps, parts, part_rows, columns), bf16),
            pltpu.VMEM((steps, width, columns), bf16),
            pltpu.VMEM((steps, width, columns), f32),
            pltpu.VMEM((steps, CORES, tall_rows, columns), bf16),
            pltpu.VMEM((panels, tall_rows, columns), bf16),
            dma((5,)),
            dma((3,)),
            dma((3,)),
            dma((steps, parts // CORES)),
            dma((batches, panels.bit_length(), parts // CORES)),
            dma((steps, parts)),
            dma((steps, parts)),
            dma((steps, parts, panels.bit_length())),
            dma((steps, parts)),
            dma((steps,)),
            dma((steps,)),
            dma((steps, CORES)),
            dma((panels,)),
        ],
        compiler_params=pltpu.CompilerParams(
            collective_id=0, has_side_effects=True, vmem_limit_bytes=67_043_328
        ),
    )(rhs_diag, rhs_tall[0], diag_inverse[0], coupling[0], tall_blocks[0].reshape(tall_rows, width), mask)
    return sol[None], res[None]


def fits_chain(mesh, rhs_diag, rhs_tall, diag_inverse, coupling, tall_blocks):
    panels, rows = mesh.shape["panel"], mesh.shape["rows"]
    return (
        rows == CORES * panels
        and rhs_diag.shape[1] == panels * diag_inverse.shape[1]
        and rhs_diag.shape[0] == panels
        and panels % CORES == 0
        and panels & (panels - 1) == 0
        and tall_blocks.shape[1] * tall_blocks.shape[2] == rhs_diag.shape[1]
    )


def shifted(block, axis, distance):
    devices = range(lax.axis_size(axis))
    route = [(i - distance, i) for i in devices if i - distance in devices]
    return lax.ppermute(block, axis, route)


def per_device(rhs_diag, rhs_tall, diag_inverse, coupling, tall_blocks, sparsity):
    panel_index = lax.axis_index("panel")
    rows_index = lax.axis_index("rows")
    panel_count = lax.axis_size("panel")
    rows_count = lax.axis_size("rows")
    batches, rows_here, columns = rhs_diag.shape
    panel_width = diag_inverse.shape[1]
    slice_rows = panel_width // rows_count
    blocks_here = tall_blocks.shape[1]
    block_rows = tall_blocks.shape[2]
    tall_rows = blocks_here * block_rows
    rows_panel = rows_index * rows_here // panel_width
    offset = jnp.clip(
        rows_index * rows_here - panel_index * panel_width, 0, panel_width - rows_here
    )
    inverse_cols = lax.dynamic_slice_in_dim(diag_inverse[0], offset, rows_here, 1)
    owner = rows_panel == panel_index
    is_later = rows_panel > panel_index
    coupling_here = coupling[0]
    tall_matrix = tall_blocks[0].reshape(tall_rows, panel_width)
    block_mask = jnp.repeat(sparsity[:, 0].astype(jnp.float32), block_rows)[:, None]

    def advance(tick_number, state_now):
        incoming, solutions, stored = state_now
        batch_now = tick_number - panel_index
        active = (batch_now >= 0) & (batch_now < batches)
        batch_safe = jnp.clip(batch_now, 0, batches - 1)
        rhs_now = lax.dynamic_index_in_dim(rhs_diag, batch_safe, 0, keepdims=False).astype(
            jnp.float32
        )
        reduced = (rhs_now - incoming).astype(jnp.bfloat16)
        partial_value = jnp.dot(inverse_cols, reduced, preferred_element_type=jnp.float32)
        partial_value = jnp.where(owner, partial_value, jnp.float32(0.0))
        own_rows = lax.psum_scatter(partial_value, "rows", scatter_dimension=0, tiled=True)
        solved = lax.all_gather(own_rows.astype(jnp.bfloat16), "rows", axis=0, tiled=True)
        previous = lax.dynamic_index_in_dim(solutions, batch_safe, 0, keepdims=False)
        solutions = lax.dynamic_update_index_in_dim(
            solutions, jnp.where(active, own_rows, previous), batch_safe, 0
        )
        update = jnp.dot(coupling_here, solved, preferred_element_type=jnp.float32)
        outgoing = incoming + jnp.where(is_later, update, jnp.float32(0.0))
        earlier = lax.dynamic_index_in_dim(stored, batch_safe, 0, keepdims=False)
        stored = lax.dynamic_update_index_in_dim(
            stored, jnp.where(active, solved, earlier), batch_safe, 0
        )
        incoming = shifted(outgoing, "panel", 1)
        return (incoming, solutions, stored)

    stored = jnp.zeros((batches, panel_width, columns), jnp.bfloat16)
    initial = (
        jnp.zeros((rows_here, columns), jnp.float32),
        jnp.zeros((batches, slice_rows, columns), jnp.float32),
        stored,
    )
    tick_count = batches + panel_count - 1
    incoming, solutions, stored = lax.fori_loop(0, tick_count, advance, initial)
    tall_terms = (
        jnp.einsum("rw,bws->brs", tall_matrix, stored, preferred_element_type=jnp.float32)
        * block_mask
    )
    summed = lax.psum_scatter(tall_terms, "panel", scatter_dimension=0, tiled=True)
    tall_residual = rhs_tall.astype(jnp.float32) - summed
    return (solutions[None], tall_residual)


def solution(mesh):
    placed = (
        P(None, "rows", None),
        P("panel", "rows", None),
        P("panel", None, None),
        P("panel", "rows", None),
        P("panel", "rows", None, None),
        P("rows", "panel"),
    )

    def run(*arrays):
        body = chained if fits_chain(mesh, *arrays[:5]) else per_device
        return jax.shard_map(
            body,
            mesh=mesh,
            in_specs=placed,
            out_specs=(P("panel", None, "rows", None), P("panel", "rows", None)),
            check_vma=False,
        )(*arrays)

    return run
```

```python
import functools

import jax
import jax.numpy as jnp
from jax import lax
from jax.experimental import pallas as pl
from jax.experimental.pallas import tpu as pltpu
from jax.sharding import PartitionSpec as P

MESH = pl.DeviceIdType.MESH
CORES = 2


def chain_kernel(
    panels, rhs_ref, tall_rhs_ref, inverse_ref, coupling_ref, tall_ref, flag_ref,
    sol_ref, res_ref,
    inv, cpl, tal, msk, rhs, rbuf, tbuf, obuf, xs, xf, ysend, ybuf,
    load_sem, sib_send, sib_recv, swap_send, first_send, r_sem, t_sem, relay_send, up_send,
    sol_send, sol_recv, y_send, y_recv,
):
    p = lax.axis_index("panel")
    r = lax.axis_index("rows")
    c = lax.rem(r, CORES)
    j = lax.div(r, CORES)
    sib = r + 1 - 2 * c
    batches, half, _ = rhs_ref.shape
    chips = panels
    steps = batches // CORES
    parts, part_rows = rbuf.shape[1:3]
    own_parts = parts // CORES
    levels = chips.bit_length() - 1
    own_rows = sol_ref.shape[1]
    blocks = flag_ref.shape[0]
    pair = 2
    last = panels - 1
    chain = j > p
    feeds_next = j == p + 1
    next_p = jnp.minimum(p + 1, last)
    next_root = jnp.minimum(p + 2, last)
    root = jnp.where(p == 0, 0, jnp.minimum(p + 1, last))
    place = jnp.bitwise_xor(j, root)
    first = jnp.logical_and(p == 0, j == 0)
    later = jnp.logical_and(p == 0, j > 0)

    def send(src, dst, ssem, rsem, panel, row):
        return pltpu.make_async_remote_copy(
            src_ref=src, dst_ref=dst, send_sem=ssem, recv_sem=rsem,
            device_id=(panel, row), device_id_type=MESH,
        )

    load_inv = pltpu.make_async_copy(inverse_ref, inv, load_sem.at[0])
    load_cpl = pltpu.make_async_copy(coupling_ref, cpl.at[c], load_sem.at[1])
    load_tal = pltpu.make_async_copy(tall_ref, tal.at[c], load_sem.at[2])
    flags = flag_ref[...].astype(jnp.float32)
    for b in range(blocks):
        msk[c, b] = jnp.broadcast_to(flags[b:b + 1, 0:1], msk.shape[2:])
    load_rhs = pltpu.make_async_copy(tall_rhs_ref, rhs, load_sem.at[3])

    def own_rhs(s, i, into, sem):
        part = c * own_parts + i
        return pltpu.make_async_copy(
            rhs_ref.at[CORES * s + c, pl.ds(i * part_rows, part_rows)], into.at[s, part], sem.at[s, part]
        )

    pieces = [(s, i) for s in range(steps) for i in range(own_parts)]

    @pl.when(first)
    def _():
        for s, i in pieces:
            own_rhs(s, i, rbuf, r_sem).start()

    @pl.when(later)
    def _():
        for s, i in pieces:
            own_rhs(s, i, tbuf, t_sem).start()

    for load in (load_inv, load_cpl, load_tal, load_rhs):
        load.start()

    barrier = pltpu.get_barrier_semaphore()
    for q in range(panels):
        for k in range(CORES):
            @pl.when(jnp.logical_or(q != p, k != c))
            def _():
                pl.semaphore_signal(barrier, inc=1, device_id=(q, CORES * j + k), device_id_type=MESH)
    for i in range(chips):
        for k in range(CORES):
            @pl.when(i != j)
            def _():
                pl.semaphore_signal(barrier, inc=1, device_id=(p, CORES * i + k), device_id_type=MESH)
    leaves = jnp.logical_and(feeds_next, next_root != j)
    enters = jnp.logical_and(jnp.logical_and(p > 0, j == root), root != p)

    @pl.when(leaves)
    def _():
        pl.semaphore_signal(barrier, inc=1, device_id=(next_p, CORES * next_root + c), device_id_type=MESH)

    @pl.when(enters)
    def _():
        pl.semaphore_signal(barrier, inc=1, device_id=(jnp.maximum(p - 1, 0), CORES * p + c), device_id_type=MESH)

    pl.semaphore_wait(
        barrier,
        CORES * panels - 1 + CORES * (chips - 1) + leaves.astype(jnp.int32) + enters.astype(jnp.int32),
    )

    def rhs_swap(s, i, into, sem):
        part = c * own_parts + i
        return send(
            rhs_ref.at[CORES * s + 1 - c, pl.ds(i * part_rows, part_rows)], into.at[s, part],
            swap_send.at[s, i], sem.at[s, part], p, sib,
        )

    def outward(k, level, i):
        part = c * own_parts + i
        return send(
            rhs_ref.at[k, pl.ds(i * part_rows, part_rows)], rbuf.at[k // CORES, part],
            first_send.at[k, level, i], r_sem.at[k // CORES, part], p, (CORES << level) + k % CORES,
        )

    outwards = [(k, n, i) for k in range(batches) for n in range(levels) for i in range(own_parts)]

    @pl.when(first)
    def _():
        for k, level, i in outwards:
            outward(k, level, i).start()
        for s, i in pieces:
            rhs_swap(s, i, rbuf, r_sem).start()

    @pl.when(later)
    def _():
        for s, i in pieces:
            rhs_swap(s, i, tbuf, t_sem).start()

    swap_cpl = send(coupling_ref, cpl.at[c], sib_send.at[0], sib_recv.at[0], p, sib)
    swap_tal = send(tall_ref, tal.at[c], sib_send.at[1], sib_recv.at[1], p, sib)
    swap_msk = send(msk.at[c], msk.at[c], sib_send.at[2], sib_recv.at[2], p, sib)
    for swap in (swap_cpl, swap_msk, swap_tal):
        swap.start()

    def arrived(ref, sem):
        pltpu.make_async_copy(ref, ref, sem).wait()

    def relay(s, part, level):
        chip = jnp.bitwise_xor(j, 1 << level)
        return send(
            rbuf.at[s, part], rbuf.at[s, part], relay_send.at[s, part, level], r_sem.at[s, part],
            p, CORES * chip + c,
        )

    def relays(level):
        return jnp.logical_and(lax.rem(place, 2 << level) == 0, jnp.logical_not(first))

    def ahead(s, part):
        return send(
            obuf.at[s, part], rbuf.at[s, part], up_send.at[s, part], r_sem.at[s, part],
            next_p, CORES * next_root + c,
        )

    def up(s, part):
        return send(obuf.at[s, part], tbuf.at[s, part], up_send.at[s, part], t_sem.at[s, part], next_p, r)

    def sol_copy(s):
        return send(
            xf.at[s, pl.ds(pl.multiple_of(sib * own_rows, own_rows), own_rows)],
            sol_ref.at[CORES * s + c], sol_send.at[s], sol_recv.at[s], p, sib,
        )

    def y_copy(s, h):
        return send(ysend.at[s, h], ybuf.at[p], y_send.at[s, h], y_recv.at[p], CORES * s + c, CORES * j + h)

    def y_local(s, h):
        return jnp.logical_and(CORES * s + c == p, c == h)

    def tall_part(s):
        for h in range(CORES):
            prod = jnp.dot(tal[h], xs[s], preferred_element_type=jnp.float32)
            prod = prod.reshape(blocks, half // blocks, prod.shape[1]) * msk[h][:, 0:1, :]
            ysend[s, h] = prod.reshape(half, prod.shape[2]).astype(jnp.bfloat16)

            @pl.when(jnp.logical_not(y_local(s, h)))
            def _():
                y_copy(s, h).start()

            @pl.when(y_local(s, h))
            def _():
                ybuf[p] = ysend[s, h]

    load_inv.wait()
    for s in range(steps):
        for part in range(parts):
            arrived(rbuf.at[s, part], r_sem.at[s, part])
            for level in range(levels):
                @pl.when(relays(level))
                def _():
                    relay(s, part, level).start()

            if part % pair == pair - 1:
                start = part + 1 - pair
                x = jnp.dot(
                    inv[:, start * part_rows:(part + 1) * part_rows],
                    rbuf[s, start:part + 1].reshape(pair * part_rows, rbuf.shape[3]),
                    preferred_element_type=jnp.float32,
                )
                xf[s] = x if start == 0 else xf[s] + x
        xs[s] = xf[s].astype(jnp.bfloat16)

        if s == 0:
            load_cpl.wait()
            swap_cpl.wait_recv()

        @pl.when(chain)
        def _():
            for start in range(0, parts, pair):
                h, i = divmod(start, own_parts)
                both = range(start, start + pair)
                for part in both:
                    arrived(tbuf.at[s, part], t_sem.at[s, part])
                update = jnp.dot(
                    cpl[h, i * part_rows:(i + pair) * part_rows], xs[s], preferred_element_type=jnp.float32
                ).reshape(pair, part_rows, xs.shape[2])
                for n, part in enumerate(both):
                    obuf[s, part] = (tbuf[s, part].astype(jnp.float32) - update[n]).astype(jnp.bfloat16)

                @pl.when(feeds_next)
                def _():
                    for part in both:
                        ahead(s, part).start()

                @pl.when(jnp.logical_not(feeds_next))
                def _():
                    for part in both:
                        up(s, part).start()

        if s == 0:
            load_tal.wait()
            swap_tal.wait_recv()
            swap_msk.wait_recv()

        sol_ref[CORES * s + c] = xf[s, pl.ds(pl.multiple_of(r * own_rows, own_rows), own_rows)]
        sol_copy(s).start()

        @pl.when(jnp.logical_not(chain))
        def _():
            tall_part(s)

    @pl.when(chain)
    def _():
        for s in range(steps):
            tall_part(s)

    load_rhs.wait()
    total = rhs[...].astype(jnp.float32)
    for q in range(panels):
        @pl.when(jnp.logical_not(jnp.logical_and(q == p, c == lax.rem(p, CORES))))
        def _():
            arrived(ybuf.at[q], y_recv.at[q])
    for q in range(panels):
        total = total - ybuf[q].astype(jnp.float32)
    res_ref[...] = total

    @pl.when(p == 0)
    def _():
        for s, i in pieces:
            rhs_swap(s, i, rbuf, r_sem).wait_send()

    @pl.when(first)
    def _():
        for k, level, i in outwards:
            outward(k, level, i).wait_send()

    for swap in (swap_cpl, swap_msk, swap_tal):
        swap.wait_send()
    for s in range(steps):
        sol_copy(s).wait_send()
        arrived(sol_ref.at[CORES * s + 1 - c], sol_recv.at[s])
        for part in range(parts):
            for level in range(levels):
                @pl.when(relays(level))
                def _():
                    relay(s, part, level).wait_send()

            @pl.when(chain)
            def _():
                ahead(s, part).wait_send()

        for h in range(CORES):
            @pl.when(jnp.logical_not(y_local(s, h)))
            def _():
                y_copy(s, h).wait_send()


def chained(rhs_diag, rhs_tall, diag_inverse, coupling, tall_blocks, sparsity):
    panels = lax.axis_size("panel")
    batches, half, columns = rhs_diag.shape
    width = diag_inverse.shape[1]
    own_rows = width // lax.axis_size("rows")
    blocks, block_rows = tall_blocks.shape[1:3]
    tall_rows = blocks * block_rows
    steps = batches // CORES
    parts = 4 * CORES
    part_rows = width // parts
    anywhere = pl.BlockSpec(memory_space=pltpu.HBM)
    inside = pl.BlockSpec(memory_space=pltpu.VMEM)
    bf16, f32 = jnp.bfloat16, jnp.float32
    dma = pltpu.SemaphoreType.DMA
    sol, res = pl.pallas_call(
        functools.partial(chain_kernel, panels),
        out_shape=(
            jax.ShapeDtypeStruct((batches, own_rows, columns), f32),
            jax.ShapeDtypeStruct((tall_rows, columns), f32),
        ),
        in_specs=[anywhere] * 5 + [inside],
        out_specs=(inside, inside),
        scratch_shapes=[
            pltpu.VMEM((width, width), bf16),
            pltpu.VMEM((CORES, half, width), bf16),
            pltpu.VMEM((CORES, tall_rows, width), bf16),
            pltpu.VMEM((CORES, blocks, 8, columns), f32),
            pltpu.VMEM((tall_rows, columns), bf16),
            pltpu.VMEM((steps, parts, part_rows, columns), bf16),
            pltpu.VMEM((steps, parts, part_rows, columns), bf16),
            pltpu.VMEM((steps, parts, part_rows, columns), bf16),
            pltpu.VMEM((steps, width, columns), bf16),
            pltpu.VMEM((steps, width, columns), f32),
            pltpu.VMEM((steps, CORES, tall_rows, columns), bf16),
            pltpu.VMEM((panels, tall_rows, columns), bf16),
            dma((4,)),
            dma((3,)),
            dma((3,)),
            dma((steps, parts // CORES)),
            dma((batches, panels.bit_length(), parts // CORES)),
            dma((steps, parts)),
            dma((steps, parts)),
            dma((steps, parts, panels.bit_length())),
            dma((steps, parts)),
            dma((steps,)),
            dma((steps,)),
            dma((steps, CORES)),
            dma((panels,)),
        ],
        compiler_params=pltpu.CompilerParams(
            collective_id=0, has_side_effects=True, vmem_limit_bytes=67_043_328
        ),
    )(rhs_diag, rhs_tall[0], diag_inverse[0], coupling[0], tall_blocks[0].reshape(tall_rows, width), sparsity)
    return sol[None], res[None]


def fits_chain(mesh, rhs_diag, rhs_tall, diag_inverse, coupling, tall_blocks):
    panels, rows = mesh.shape["panel"], mesh.shape["rows"]
    return (
        rows == CORES * panels
        and rhs_diag.shape[1] == panels * diag_inverse.shape[1]
        and rhs_diag.shape[0] == panels
        and panels % CORES == 0
        and panels & (panels - 1) == 0
        and tall_blocks.shape[1] * tall_blocks.shape[2] == rhs_diag.shape[1]
    )


def shifted(block, axis, distance):
    devices = range(lax.axis_size(axis))
    route = [(i - distance, i) for i in devices if i - distance in devices]
    return lax.ppermute(block, axis, route)


def per_device(rhs_diag, rhs_tall, diag_inverse, coupling, tall_blocks, sparsity):
    panel_index = lax.axis_index("panel")
    rows_index = lax.axis_index("rows")
    panel_count = lax.axis_size("panel")
    rows_count = lax.axis_size("rows")
    batches, rows_here, columns = rhs_diag.shape
    panel_width = diag_inverse.shape[1]
    slice_rows = panel_width // rows_count
    blocks_here = tall_blocks.shape[1]
    block_rows = tall_blocks.shape[2]
    tall_rows = blocks_here * block_rows
    rows_panel = rows_index * rows_here // panel_width
    offset = jnp.clip(
        rows_index * rows_here - panel_index * panel_width, 0, panel_width - rows_here
    )
    inverse_cols = lax.dynamic_slice_in_dim(diag_inverse[0], offset, rows_here, 1)
    owner = rows_panel == panel_index
    is_later = rows_panel > panel_index
    coupling_here = coupling[0]
    tall_matrix = tall_blocks[0].reshape(tall_rows, panel_width)
    block_mask = jnp.repeat(sparsity[:, 0].astype(jnp.float32), block_rows)[:, None]

    def advance(tick_number, state_now):
        incoming, solutions, stored = state_now
        batch_now = tick_number - panel_index
        active = (batch_now >= 0) & (batch_now < batches)
        batch_safe = jnp.clip(batch_now, 0, batches - 1)
        rhs_now = lax.dynamic_index_in_dim(rhs_diag, batch_safe, 0, keepdims=False).astype(
            jnp.float32
        )
        reduced = (rhs_now - incoming).astype(jnp.bfloat16)
        partial_value = jnp.dot(inverse_cols, reduced, preferred_element_type=jnp.float32)
        partial_value = jnp.where(owner, partial_value, jnp.float32(0.0))
        own_rows = lax.psum_scatter(partial_value, "rows", scatter_dimension=0, tiled=True)
        solved = lax.all_gather(own_rows.astype(jnp.bfloat16), "rows", axis=0, tiled=True)
        previous = lax.dynamic_index_in_dim(solutions, batch_safe, 0, keepdims=False)
        solutions = lax.dynamic_update_index_in_dim(
            solutions, jnp.where(active, own_rows, previous), batch_safe, 0
        )
        update = jnp.dot(coupling_here, solved, preferred_element_type=jnp.float32)
        outgoing = incoming + jnp.where(is_later, update, jnp.float32(0.0))
        earlier = lax.dynamic_index_in_dim(stored, batch_safe, 0, keepdims=False)
        stored = lax.dynamic_update_index_in_dim(
            stored, jnp.where(active, solved, earlier), batch_safe, 0
        )
        incoming = shifted(outgoing, "panel", 1)
        return (incoming, solutions, stored)

    stored = jnp.zeros((batches, panel_width, columns), jnp.bfloat16)
    initial = (
        jnp.zeros((rows_here, columns), jnp.float32),
        jnp.zeros((batches, slice_rows, columns), jnp.float32),
        stored,
    )
    tick_count = batches + panel_count - 1
    incoming, solutions, stored = lax.fori_loop(0, tick_count, advance, initial)
    tall_terms = (
        jnp.einsum("rw,bws->brs", tall_matrix, stored, preferred_element_type=jnp.float32)
        * block_mask
    )
    summed = lax.psum_scatter(tall_terms, "panel", scatter_dimension=0, tiled=True)
    tall_residual = rhs_tall.astype(jnp.float32) - summed
    return (solutions[None], tall_residual)


def solution(mesh):
    placed = (
        P(None, "rows", None),
        P("panel", "rows", None),
        P("panel", None, None),
        P("panel", "rows", None),
        P("panel", "rows", None, None),
        P("rows", "panel"),
    )

    def run(*arrays):
        body = chained if fits_chain(mesh, *arrays[:5]) else per_device
        return jax.shard_map(
            body,
            mesh=mesh,
            in_specs=placed,
            out_specs=(P("panel", None, "rows", None), P("panel", "rows", None)),
            check_vma=False,
        )(*arrays)

    return run
```

```python
import functools

import jax
import jax.numpy as jnp
from jax import lax
from jax.experimental import pallas as pl
from jax.experimental.pallas import tpu as pltpu
from jax.sharding import PartitionSpec as P

MESH = pl.DeviceIdType.MESH
CORES = 2


def chain_kernel(
    panels, rhs_ref, tall_rhs_ref, inverse_ref, coupling_ref, tall_ref, flag_ref,
    sol_ref, res_ref,
    inv, cpl, tal, msk, rhs, rbuf, tbuf, obuf, xs, xf, ysend, ybuf,
    load_sem, sib_send, sib_recv, swap_send, first_send, r_sem, t_sem, relay_send, up_send,
    sol_send, sol_recv, y_send, y_recv,
):
    p = lax.axis_index("panel")
    r = lax.axis_index("rows")
    c = lax.rem(r, CORES)
    j = lax.div(r, CORES)
    sib = r + 1 - 2 * c
    batches, half, _ = rhs_ref.shape
    chips = panels
    steps = batches // CORES
    parts, part_rows = rbuf.shape[1:3]
    own_parts = parts // CORES
    levels = chips.bit_length() - 1
    own_rows = sol_ref.shape[1]
    blocks = flag_ref.shape[0]
    pair = 1
    last = panels - 1
    chain = j > p
    feeds_next = j == p + 1
    next_p = jnp.minimum(p + 1, last)
    next_root = jnp.minimum(p + 2, last)
    root = jnp.where(p == 0, 0, jnp.minimum(p + 1, last))
    place = jnp.bitwise_xor(j, root)
    first = jnp.logical_and(p == 0, j == 0)
    later = jnp.logical_and(p == 0, j > 0)

    def send(src, dst, ssem, rsem, panel, row):
        return pltpu.make_async_remote_copy(
            src_ref=src, dst_ref=dst, send_sem=ssem, recv_sem=rsem,
            device_id=(panel, row), device_id_type=MESH,
        )

    load_inv = pltpu.make_async_copy(inverse_ref, inv, load_sem.at[0])
    load_cpl = pltpu.make_async_copy(coupling_ref, cpl.at[c], load_sem.at[1])
    load_tal = pltpu.make_async_copy(tall_ref, tal.at[c], load_sem.at[2])
    flags = flag_ref[...].astype(jnp.float32)
    for b in range(blocks):
        msk[c, b] = jnp.broadcast_to(flags[b:b + 1, 0:1], msk.shape[2:])
    load_rhs = pltpu.make_async_copy(tall_rhs_ref, rhs, load_sem.at[3])

    def own_rhs(s, i, into, sem):
        part = c * own_parts + i
        return pltpu.make_async_copy(
            rhs_ref.at[CORES * s + c, pl.ds(i * part_rows, part_rows)], into.at[s, part], sem.at[s, part]
        )

    pieces = [(s, i) for s in range(steps) for i in range(own_parts)]

    @pl.when(first)
    def _():
        for s, i in pieces:
            own_rhs(s, i, rbuf, r_sem).start()

    @pl.when(later)
    def _():
        for s, i in pieces:
            own_rhs(s, i, tbuf, t_sem).start()

    for load in (load_inv, load_cpl, load_tal, load_rhs):
        load.start()

    barrier = pltpu.get_barrier_semaphore()
    for q in range(panels):
        for k in range(CORES):
            @pl.when(jnp.logical_or(q != p, k != c))
            def _():
                pl.semaphore_signal(barrier, inc=1, device_id=(q, CORES * j + k), device_id_type=MESH)
    for i in range(chips):
        for k in range(CORES):
            @pl.when(i != j)
            def _():
                pl.semaphore_signal(barrier, inc=1, device_id=(p, CORES * i + k), device_id_type=MESH)
    leaves = jnp.logical_and(feeds_next, next_root != j)
    enters = jnp.logical_and(jnp.logical_and(p > 0, j == root), root != p)

    @pl.when(leaves)
    def _():
        pl.semaphore_signal(barrier, inc=1, device_id=(next_p, CORES * next_root + c), device_id_type=MESH)

    @pl.when(enters)
    def _():
        pl.semaphore_signal(barrier, inc=1, device_id=(jnp.maximum(p - 1, 0), CORES * p + c), device_id_type=MESH)

    pl.semaphore_wait(
        barrier,
        CORES * panels - 1 + CORES * (chips - 1) + leaves.astype(jnp.int32) + enters.astype(jnp.int32),
    )

    def rhs_swap(s, i, into, sem):
        part = c * own_parts + i
        return send(
            rhs_ref.at[CORES * s + 1 - c, pl.ds(i * part_rows, part_rows)], into.at[s, part],
            swap_send.at[s, i], sem.at[s, part], p, sib,
        )

    def outward(k, level, i):
        part = c * own_parts + i
        return send(
            rhs_ref.at[k, pl.ds(i * part_rows, part_rows)], rbuf.at[k // CORES, part],
            first_send.at[k, level, i], r_sem.at[k // CORES, part], p, (CORES << level) + k % CORES,
        )

    outwards = [(k, n, i) for k in range(batches) for n in range(levels) for i in range(own_parts)]

    @pl.when(first)
    def _():
        for k, level, i in outwards:
            outward(k, level, i).start()
        for s, i in pieces:
            rhs_swap(s, i, rbuf, r_sem).start()

    @pl.when(later)
    def _():
        for s, i in pieces:
            rhs_swap(s, i, tbuf, t_sem).start()

    swap_cpl = send(coupling_ref, cpl.at[c], sib_send.at[0], sib_recv.at[0], p, sib)
    swap_tal = send(tall_ref, tal.at[c], sib_send.at[1], sib_recv.at[1], p, sib)
    swap_msk = send(msk.at[c], msk.at[c], sib_send.at[2], sib_recv.at[2], p, sib)
    for swap in (swap_cpl, swap_msk, swap_tal):
        swap.start()

    def arrived(ref, sem):
        pltpu.make_async_copy(ref, ref, sem).wait()

    def relay(s, part, level):
        chip = jnp.bitwise_xor(j, 1 << level)
        return send(
            rbuf.at[s, part], rbuf.at[s, part], relay_send.at[s, part, level], r_sem.at[s, part],
            p, CORES * chip + c,
        )

    def relays(level):
        return jnp.logical_and(lax.rem(place, 2 << level) == 0, jnp.logical_not(first))

    def ahead(s, part):
        return send(
            obuf.at[s, part], rbuf.at[s, part], up_send.at[s, part], r_sem.at[s, part],
            next_p, CORES * next_root + c,
        )

    def up(s, part):
        return send(obuf.at[s, part], tbuf.at[s, part], up_send.at[s, part], t_sem.at[s, part], next_p, r)

    def sol_copy(s):
        return send(
            xf.at[s, pl.ds(pl.multiple_of(sib * own_rows, own_rows), own_rows)],
            sol_ref.at[CORES * s + c], sol_send.at[s], sol_recv.at[s], p, sib,
        )

    def y_copy(s, h):
        return send(ysend.at[s, h], ybuf.at[p], y_send.at[s, h], y_recv.at[p], CORES * s + c, CORES * j + h)

    def y_local(s, h):
        return jnp.logical_and(CORES * s + c == p, c == h)

    def tall_part(s):
        for h in range(CORES):
            prod = jnp.dot(tal[h], xs[s], preferred_element_type=jnp.float32)
            prod = prod.reshape(blocks, half // blocks, prod.shape[1]) * msk[h][:, 0:1, :]
            ysend[s, h] = prod.reshape(half, prod.shape[2]).astype(jnp.bfloat16)

            @pl.when(jnp.logical_not(y_local(s, h)))
            def _():
                y_copy(s, h).start()

            @pl.when(y_local(s, h))
            def _():
                ybuf[p] = ysend[s, h]

    load_inv.wait()
    for s in range(steps):
        for part in range(parts):
            arrived(rbuf.at[s, part], r_sem.at[s, part])
            for level in range(levels):
                @pl.when(relays(level))
                def _():
                    relay(s, part, level).start()

            if part % pair == pair - 1:
                start = part + 1 - pair
                x = jnp.dot(
                    inv[:, start * part_rows:(part + 1) * part_rows],
                    rbuf[s, start:part + 1].reshape(pair * part_rows, rbuf.shape[3]),
                    preferred_element_type=jnp.float32,
                )
                xf[s] = x if start == 0 else xf[s] + x
        xs[s] = xf[s].astype(jnp.bfloat16)

        if s == 0:
            load_cpl.wait()
            swap_cpl.wait_recv()

        @pl.when(chain)
        def _():
            for start in range(0, parts, pair):
                h, i = divmod(start, own_parts)
                both = range(start, start + pair)
                for part in both:
                    arrived(tbuf.at[s, part], t_sem.at[s, part])
                update = jnp.dot(
                    cpl[h, i * part_rows:(i + pair) * part_rows], xs[s], preferred_element_type=jnp.float32
                ).reshape(pair, part_rows, xs.shape[2])
                for n, part in enumerate(both):
                    obuf[s, part] = (tbuf[s, part].astype(jnp.float32) - update[n]).astype(jnp.bfloat16)

                @pl.when(feeds_next)
                def _():
                    for part in both:
                        ahead(s, part).start()

                @pl.when(jnp.logical_not(feeds_next))
                def _():
                    for part in both:
                        up(s, part).start()

        if s == 0:
            load_tal.wait()
            swap_tal.wait_recv()
            swap_msk.wait_recv()

        sol_ref[CORES * s + c] = xf[s, pl.ds(pl.multiple_of(r * own_rows, own_rows), own_rows)]
        sol_copy(s).start()

        @pl.when(jnp.logical_not(chain))
        def _():
            tall_part(s)

    @pl.when(chain)
    def _():
        for s in range(steps):
            tall_part(s)

    load_rhs.wait()
    total = rhs[...].astype(jnp.float32)
    for q in range(panels):
        @pl.when(jnp.logical_not(jnp.logical_and(q == p, c == lax.rem(p, CORES))))
        def _():
            arrived(ybuf.at[q], y_recv.at[q])
    for q in range(panels):
        total = total - ybuf[q].astype(jnp.float32)
    res_ref[...] = total

    @pl.when(p == 0)
    def _():
        for s, i in pieces:
            rhs_swap(s, i, rbuf, r_sem).wait_send()

    @pl.when(first)
    def _():
        for k, level, i in outwards:
            outward(k, level, i).wait_send()

    for swap in (swap_cpl, swap_msk, swap_tal):
        swap.wait_send()
    for s in range(steps):
        sol_copy(s).wait_send()
        arrived(sol_ref.at[CORES * s + 1 - c], sol_recv.at[s])
        for part in range(parts):
            for level in range(levels):
                @pl.when(relays(level))
                def _():
                    relay(s, part, level).wait_send()

            @pl.when(chain)
            def _():
                ahead(s, part).wait_send()

        for h in range(CORES):
            @pl.when(jnp.logical_not(y_local(s, h)))
            def _():
                y_copy(s, h).wait_send()


def chained(rhs_diag, rhs_tall, diag_inverse, coupling, tall_blocks, sparsity):
    panels = lax.axis_size("panel")
    batches, half, columns = rhs_diag.shape
    width = diag_inverse.shape[1]
    own_rows = width // lax.axis_size("rows")
    blocks, block_rows = tall_blocks.shape[1:3]
    tall_rows = blocks * block_rows
    steps = batches // CORES
    parts = 2 * CORES
    part_rows = width // parts
    anywhere = pl.BlockSpec(memory_space=pltpu.HBM)
    inside = pl.BlockSpec(memory_space=pltpu.VMEM)
    bf16, f32 = jnp.bfloat16, jnp.float32
    dma = pltpu.SemaphoreType.DMA
    sol, res = pl.pallas_call(
        functools.partial(chain_kernel, panels),
        out_shape=(
            jax.ShapeDtypeStruct((batches, own_rows, columns), f32),
            jax.ShapeDtypeStruct((tall_rows, columns), f32),
        ),
        in_specs=[anywhere] * 5 + [inside],
        out_specs=(inside, inside),
        scratch_shapes=[
            pltpu.VMEM((width, width), bf16),
            pltpu.VMEM((CORES, half, width), bf16),
            pltpu.VMEM((CORES, tall_rows, width), bf16),
            pltpu.VMEM((CORES, blocks, 8, columns), f32),
            pltpu.VMEM((tall_rows, columns), bf16),
            pltpu.VMEM((steps, parts, part_rows, columns), bf16),
            pltpu.VMEM((steps, parts, part_rows, columns), bf16),
            pltpu.VMEM((steps, parts, part_rows, columns), bf16),
            pltpu.VMEM((steps, width, columns), bf16),
            pltpu.VMEM((steps, width, columns), f32),
            pltpu.VMEM((steps, CORES, tall_rows, columns), bf16),
            pltpu.VMEM((panels, tall_rows, columns), bf16),
            dma((4,)),
            dma((3,)),
            dma((3,)),
            dma((steps, parts // CORES)),
            dma((batches, panels.bit_length(), parts // CORES)),
            dma((steps, parts)),
            dma((steps, parts)),
            dma((steps, parts, panels.bit_length())),
            dma((steps, parts)),
            dma((steps,)),
            dma((steps,)),
            dma((steps, CORES)),
            dma((panels,)),
        ],
        compiler_params=pltpu.CompilerParams(
            collective_id=0, has_side_effects=True, vmem_limit_bytes=67_043_328
        ),
    )(rhs_diag, rhs_tall[0], diag_inverse[0], coupling[0], tall_blocks[0].reshape(tall_rows, width), sparsity)
    return sol[None], res[None]


def fits_chain(mesh, rhs_diag, rhs_tall, diag_inverse, coupling, tall_blocks):
    panels, rows = mesh.shape["panel"], mesh.shape["rows"]
    return (
        rows == CORES * panels
        and rhs_diag.shape[1] == panels * diag_inverse.shape[1]
        and rhs_diag.shape[0] == panels
        and panels % CORES == 0
        and panels & (panels - 1) == 0
        and tall_blocks.shape[1] * tall_blocks.shape[2] == rhs_diag.shape[1]
    )


def shifted(block, axis, distance):
    devices = range(lax.axis_size(axis))
    route = [(i - distance, i) for i in devices if i - distance in devices]
    return lax.ppermute(block, axis, route)


def per_device(rhs_diag, rhs_tall, diag_inverse, coupling, tall_blocks, sparsity):
    panel_index = lax.axis_index("panel")
    rows_index = lax.axis_index("rows")
    panel_count = lax.axis_size("panel")
    rows_count = lax.axis_size("rows")
    batches, rows_here, columns = rhs_diag.shape
    panel_width = diag_inverse.shape[1]
    slice_rows = panel_width // rows_count
    blocks_here = tall_blocks.shape[1]
    block_rows = tall_blocks.shape[2]
    tall_rows = blocks_here * block_rows
    rows_panel = rows_index * rows_here // panel_width
    offset = jnp.clip(
        rows_index * rows_here - panel_index * panel_width, 0, panel_width - rows_here
    )
    inverse_cols = lax.dynamic_slice_in_dim(diag_inverse[0], offset, rows_here, 1)
    owner = rows_panel == panel_index
    is_later = rows_panel > panel_index
    coupling_here = coupling[0]
    tall_matrix = tall_blocks[0].reshape(tall_rows, panel_width)
    block_mask = jnp.repeat(sparsity[:, 0].astype(jnp.float32), block_rows)[:, None]

    def advance(tick_number, state_now):
        incoming, solutions, stored = state_now
        batch_now = tick_number - panel_index
        active = (batch_now >= 0) & (batch_now < batches)
        batch_safe = jnp.clip(batch_now, 0, batches - 1)
        rhs_now = lax.dynamic_index_in_dim(rhs_diag, batch_safe, 0, keepdims=False).astype(
            jnp.float32
        )
        reduced = (rhs_now - incoming).astype(jnp.bfloat16)
        partial_value = jnp.dot(inverse_cols, reduced, preferred_element_type=jnp.float32)
        partial_value = jnp.where(owner, partial_value, jnp.float32(0.0))
        own_rows = lax.psum_scatter(partial_value, "rows", scatter_dimension=0, tiled=True)
        solved = lax.all_gather(own_rows.astype(jnp.bfloat16), "rows", axis=0, tiled=True)
        previous = lax.dynamic_index_in_dim(solutions, batch_safe, 0, keepdims=False)
        solutions = lax.dynamic_update_index_in_dim(
            solutions, jnp.where(active, own_rows, previous), batch_safe, 0
        )
        update = jnp.dot(coupling_here, solved, preferred_element_type=jnp.float32)
        outgoing = incoming + jnp.where(is_later, update, jnp.float32(0.0))
        earlier = lax.dynamic_index_in_dim(stored, batch_safe, 0, keepdims=False)
        stored = lax.dynamic_update_index_in_dim(
            stored, jnp.where(active, solved, earlier), batch_safe, 0
        )
        incoming = shifted(outgoing, "panel", 1)
        return (incoming, solutions, stored)

    stored = jnp.zeros((batches, panel_width, columns), jnp.bfloat16)
    initial = (
        jnp.zeros((rows_here, columns), jnp.float32),
        jnp.zeros((batches, slice_rows, columns), jnp.float32),
        stored,
    )
    tick_count = batches + panel_count - 1
    incoming, solutions, stored = lax.fori_loop(0, tick_count, advance, initial)
    tall_terms = (
        jnp.einsum("rw,bws->brs", tall_matrix, stored, preferred_element_type=jnp.float32)
        * block_mask
    )
    summed = lax.psum_scatter(tall_terms, "panel", scatter_dimension=0, tiled=True)
    tall_residual = rhs_tall.astype(jnp.float32) - summed
    return (solutions[None], tall_residual)


def solution(mesh):
    placed = (
        P(None, "rows", None),
        P("panel", "rows", None),
        P("panel", None, None),
        P("panel", "rows", None),
        P("panel", "rows", None, None),
        P("rows", "panel"),
    )

    def run(*arrays):
        body = chained if fits_chain(mesh, *arrays[:5]) else per_device
        return jax.shard_map(
            body,
            mesh=mesh,
            in_specs=placed,
            out_specs=(P("panel", None, "rows", None), P("panel", "rows", None)),
            check_vma=False,
        )(*arrays)

    return run
```
